32 devices in a mesh: band: 2 (over x), domain: 16 (over z, y, core).
Axes of the slice: x: 2, y: 2, z: 4, core: 2. Of those that a mesh axis runs over, the one named last changes fastest.
Arguments:
- dens_part: float32 [2, 171, 36864], P('band', None, 'domain'), may hold values from -3 to 3
- counts: int32 [16], P('domain'), may hold values from 1 to 2304, 12288 in all
- gaunt: float32 [171, 525], replicated, may hold values from -0.4375 to 0.4375
- pair_waves: float32 [21, 400], replicated, may hold values from -1.25 to 1.25
- y_table: float32 [25, 50], replicated, may hold values from -1.25 to 1.25
- core: float32 [400], replicated, may hold values from 1 to 4
- radial_weights: float32 [400], replicated, may hold values from 0.0001 to 0.001
Outputs:
- dh_packed: float32 [171, 36864], P(None, 'domain')
- atom_energy: float32 [36864], P('domain')
The draws below stay inside these ranges and needn't reach their ends.
Inputs may be any that keep to these rules, and one draw needn't show every extreme that they name: `counts`: atoms owned by each domain; they sum to 12288, and some domain owns exactly 2304.
All inputs are finite; a program needn't handle non-finite values. No bound on the sum of `counts` on one device may be relied on, other than what follows from the above.
Results may differ from the reference program's by a relative error of at most 0.0003.
Values sent between devices are 32-bit elements; how exact they have to be, the bound alone decides.
A program may use at most 128 MiB of HBM per device.

```python
import math
import jax
import jax.numpy as jnp
import numpy as np
from jax import lax

NP = 171
NQ = 21
LM = 25
NDIR = 50
G = 400
ATOM_DEV = 768
SLOTS = 2304
N_BAND = 2
N_DOMAIN = 16


def block_levels(own_key, shape, shards, smallest, high):
    level = 1.0
    for position, parts in shards:
        steps = jax.random.uniform(jax.random.fold_in(jax.random.fold_in(own_key, 6), position), (parts,), jnp.float32, smallest / len(shards), high / len(shards))
        level = level * jnp.repeat(jnp.exp(steps), shape[position] // parts).reshape((-1,) + (1,) * (len(shape) - 1 - position))
    return level


def profile(amount, total, bound, skew):
    portions = [(1 << 20) // math.isqrt(grade ** skew) + 1 for grade in range(2, amount + 1)]
    rest, given = total - bound - (amount - 1), [1] * (amount - 1)
    while rest > 0:
        movable = [i for i in range(amount - 1) if given[i] < bound]
        pool, left = sum([portions[i] for i in movable]), rest
        for i in movable:
            more = min(bound - given[i], max(1, left * portions[i] // pool), rest)
            given[i] = given[i] + more
            rest = rest - more
    return np.array([bound] + given)


def ragged_sizes(own_key, count, total, limit, lean):
    if count == 2:
        one = jax.random.randint(own_key, (), max(1, total - limit), min(limit, total - 1) + 1)
        return jnp.stack([one, total - one])
    tallies = jnp.asarray(profile(count, total, limit, lean), jnp.int32)
    couples = (count - 1) // 2
    source_of, taker = tallies[1:1 + 2 * couples:2], tallies[2:2 + 2 * couples:2]
    room = jnp.minimum(source_of - 1, limit - taker)
    passed = jax.random.randint(jax.random.fold_in(own_key, 1), (couples,), 0, 1 << 20) % (room + 1)
    tallies = tallies.at[1:1 + 2 * couples:2].set(source_of - passed).at[2:2 + 2 * couples:2].set(taker + passed)
    return tallies[jax.random.permutation(jax.random.fold_in(own_key, 2), count)]


def bell_draw(rng, shape, scale, limit, split=(), held_as=jnp.bfloat16):
    array = scale * jax.random.normal(rng, shape, jnp.float32)
    if split:
        array = array * block_levels(rng, shape, split, -0.22, 0.18)
    return jnp.clip(array, -limit, limit).astype(held_as)


def setup_inputs(seed: int = 0) -> dict:
    streams_of = jax.random.split(jax.random.key(seed), 8)
    dens_part = bell_draw(streams_of[0], (N_BAND, NP, N_DOMAIN * SLOTS), 0.35, 3.0, ((0, 2), (2, 16)), jnp.float32)
    counts = ragged_sizes(streams_of[1], N_DOMAIN, ATOM_DEV * N_DOMAIN, SLOTS, 2).astype(jnp.int32)
    gaunt = bell_draw(streams_of[2], (NP, LM * NQ), NP ** -0.5, 0.4375, (), jnp.float32)
    pair_waves = bell_draw(streams_of[3], (NQ, G), NQ ** -0.5, 1.25, (), jnp.float32)
    y_table = bell_draw(streams_of[4], (LM, NDIR), LM ** -0.5, 1.25, (), jnp.float32)
    core = jnp.clip(jnp.exp(jax.random.uniform(streams_of[5], (G,), jnp.float32, math.log(1.0), math.log(4.0))), 1.0, 4.0)
    radial_weights = jnp.clip(jnp.exp(jax.random.uniform(streams_of[6], (G,), jnp.float32, math.log(0.0001), math.log(0.001))), 0.0001, 0.001)
    return {"dens_part": dens_part, "counts": counts, "gaunt": gaunt, "pair_waves": pair_waves, "y_table": y_table, "core": core, "radial_weights": radial_weights}


highest = lax.Precision.HIGHEST

def local_energy(density_rows, gaunt, pair_waves, y_table, core, radial_weights):
    atom_count = density_rows.shape[0]
    harmonics = y_table.shape[0]
    pair_count = pair_waves.shape[0]
    directions = y_table.shape[1]
    coefficients = jnp.dot(density_rows, gaunt, precision=highest, preferred_element_type=jnp.float32)
    coefficients = coefficients.reshape(atom_count * harmonics, pair_count)
    radial = jnp.dot(coefficients, pair_waves, precision=highest, preferred_element_type=jnp.float32)
    radial = radial.reshape(atom_count, harmonics, pair_waves.shape[1])
    points = jnp.einsum('ln,alg->ang', y_table, radial, precision=highest) + core[None, None, :]
    smooth = jnp.sqrt(points * points + 0.25)
    cube_root = jnp.cbrt(smooth)
    wigner_radius = 0.6203504908994 / cube_root
    denominator = 7.8 + wigner_radius
    energy_density = -0.7385587663820224 * smooth * cube_root - 0.44 * smooth / denominator
    slope = -0.9847450218426965 * cube_root - 0.44 * (1.0 / denominator + wigner_radius / (3.0 * denominator * denominator))
    point_weight = 4.0 * jnp.pi / directions * radial_weights
    energy = lax.optimization_barrier(jnp.sum(energy_density * point_weight[None, None, :], axis=(1, 2)))
    potential = point_weight[None, None, :] * slope * points / smooth
    back_radial = jnp.einsum('ln,ang->alg', y_table, potential, precision=highest)
    back_coef = jnp.dot(back_radial.reshape(atom_count * harmonics, pair_waves.shape[1]), pair_waves.T, precision=highest, preferred_element_type=jnp.float32)
    back_coef = back_coef.reshape(atom_count, harmonics * pair_count)
    hamiltonian = jnp.dot(back_coef, gaunt.T, precision=highest, preferred_element_type=jnp.float32)
    return (hamiltonian, energy)

def reference(dens_part, counts, gaunt, pair_waves, y_table, core, radial_weights):
    density = lax.optimization_barrier(jnp.sum(dens_part, axis=0)).T.reshape(N_DOMAIN, SLOTS, NP)
    slot_ids = jnp.arange(SLOTS).astype(jnp.int32)

    def per_domain(packed):
        block, owned = packed
        is_alive = slot_ids < owned
        block = jnp.where(is_alive[:, None], block, jnp.zeros_like(block))
        hamiltonian, energy = local_energy(block, gaunt, pair_waves, y_table, core, radial_weights)
        hamiltonian = jnp.where(is_alive[:, None], hamiltonian, jnp.zeros_like(hamiltonian))
        energy = jnp.where(is_alive, energy, jnp.zeros_like(energy))
        return (hamiltonian, energy)
    hamiltonian, energy = lax.map(per_domain, (density, counts.astype(jnp.int32)))
    return (hamiltonian.reshape(N_DOMAIN * SLOTS, NP).T, energy.reshape(N_DOMAIN * SLOTS))
```

```python
import math

import jax
import jax.numpy as jnp
from jax import lax
from jax.experimental import pallas as pl
from jax.experimental.pallas import tpu as pltpu
from jax.sharding import PartitionSpec as P

highest = lax.Precision.HIGHEST
f32 = jnp.float32
bf16 = jnp.bfloat16

LANES = 128
WIDE = 256

C_RS = 0.6203504908994
EX_A = 0.7385587663820224
EX_D = 0.9847450218426965

def round_up(value, step):
    return -(-value // step) * step

def split(x):
    hi = lax.reduce_precision(x, 8, 7)
    return hi.astype(bf16), (x - hi).astype(bf16)

def atom_kernel(
    dens_ref, gy_ref, gyb_ref, pw_ref, pwb_ref, core_ref, weight_ref,
    ham_ref, energy_ref, pts_ref, hi_ref, lo_ref, eacc_ref, back_ref, *, pairs, step
):
    atoms = dens_ref.shape[1]
    rows = pw_ref.shape[1]
    grid_points = pw_ref.shape[0]
    couples = gy_ref.shape[0]
    chunks = 2 * atoms // WIDE
    eacc_ref[...] = jnp.zeros_like(eacc_ref)

    def mixed(x):
        ids = lax.broadcasted_iota(jnp.int32, x.shape, 0)
        hi = x.astype(bf16).astype(f32)
        low = (ids >= pairs) & (ids < 2 * pairs)
        return jnp.where(low, x - hi, hi).astype(bf16)

    def body(m, carry):
        both = jnp.dot(gy_ref[m], dens_ref[...], preferred_element_type=f32)
        lhs = mixed(jnp.concatenate([both[:rows], both[rows:]], axis=1))
        back = []
        for j in range(chunks):
            cols = lhs[:, j * WIDE:(j + 1) * WIDE]
            pts_ref[j] = jnp.dot(pw_ref[...], cols, preferred_element_type=f32)
            for g in range(0, grid_points, step):
                part = pl.ds(g, step)
                p = pts_ref[j, part, :] + core_ref[part, :]
                u = p * p + 0.25
                v = jnp.exp2(jnp.log(u) * (-1.0 / (6.0 * math.log(2.0))))
                r = v / (7.8 + C_RS * v)
                v2 = v * v
                br = 0.44 * r
                eacc_ref[j, part, :] += (u * v2) * (EX_A + br)
                pot = (p * v2) * (EX_D + (0.44 + (0.44 * C_RS / 3.0) * r) * r)
                hi = pot.astype(bf16)
                hi_ref[j, part, :] = hi
                lo_ref[j, part, :] = (pot - hi.astype(f32)).astype(bf16)
            first = jnp.dot(pwb_ref[...], hi_ref[j], preferred_element_type=f32)
            second = jnp.dot(pwb_ref[:rows, :], lo_ref[j], preferred_element_type=f32)
            back.append(first[:rows] + first[rows:] + second)
        back = mixed(jnp.concatenate(back, axis=1))
        start = pl.multiple_of(m * 2 * rows, 2 * rows)
        back_ref[pl.ds(start, rows), :] = back[:, :atoms]
        back_ref[pl.ds(start + rows, rows), :] = back[:, atoms:]
        return carry

    lax.fori_loop(0, couples, body, 0)
    ham_ref[...] = jnp.dot(gyb_ref[...], back_ref[...], preferred_element_type=f32)
    sums = [
        jnp.sum(eacc_ref[j] * weight_ref[...], axis=0, keepdims=True) for j in range(chunks)
    ]
    sums = jnp.concatenate(sums, axis=1)
    energy_ref[...] = jnp.broadcast_to(
        -(sums[:, :atoms] + sums[:, atoms:]), energy_ref.shape
    )

def prepare(gaunt, pair_waves, y_table, core, radial_weights):
    entries = gaunt.shape[0]
    harmonics, directions = y_table.shape
    pairs, grid_points = pair_waves.shape
    rows = round_up(3 * pairs, 16)
    extra = rows - 3 * pairs
    assert directions % 2 == 0
    fused = jnp.einsum(
        "plq,ln->nqp", gaunt.reshape(entries, harmonics, pairs), y_table, precision=highest
    )

    hi, lo = split(fused)
    wide = lambda a, b, c: jnp.pad(
        jnp.concatenate([a, b, c], axis=1), ((0, 0), (0, extra), (0, 0))
    )
    hi3 = wide(hi, hi, hi)
    lo3 = wide(lo, lo, lo)
    gy = jnp.concatenate([hi3, hi3, lo3], axis=2).reshape(directions // 2, 2 * rows, 3 * entries)
    gyb = wide(hi, hi, lo).reshape(directions * rows, entries).T
    pw_hi, pw_lo = split(pair_waves)
    pw = jnp.pad(jnp.concatenate([pw_hi, pw_hi, pw_lo], axis=0), ((0, extra), (0, 0))).T
    point_weight = 4.0 * jnp.pi / directions * radial_weights
    b_hi, b_lo = split(-point_weight[None, :] * pair_waves)
    triple = lambda x: jnp.pad(jnp.concatenate([x, x, x], axis=0), ((0, extra), (0, 0)))
    pwb = jnp.concatenate([triple(b_hi), triple(b_lo)], axis=0)
    core_wide = jnp.broadcast_to(core[:, None], (grid_points, WIDE))
    weight_wide = jnp.broadcast_to(point_weight[:, None], (grid_points, WIDE))
    return gy, gyb, pw, pwb, core_wide, weight_wide

def local_energy(columns, tables, pairs):
    entries, atoms = columns.shape
    gy, gyb, pw, pwb, core_wide, weight_wide = tables
    grid_points, rows = pw.shape
    hi, lo = split(columns)
    dens = jnp.concatenate([hi, lo, hi], axis=0)
    chunks = 2 * atoms // WIDE
    step = 80 if grid_points % 80 == 0 else grid_points

    ham, energy = pl.pallas_call(
        lambda *refs: atom_kernel(*refs, pairs=pairs, step=step),
        out_shape=(
            jax.ShapeDtypeStruct((entries, atoms), f32),
            jax.ShapeDtypeStruct((8, atoms), f32),
        ),
        scratch_shapes=[
            pltpu.VMEM((chunks, grid_points, WIDE), f32),
            pltpu.VMEM((chunks, grid_points, WIDE), bf16),
            pltpu.VMEM((chunks, grid_points, WIDE), bf16),
            pltpu.VMEM((chunks, grid_points, WIDE), f32),
            pltpu.VMEM((gyb.shape[1], atoms), bf16),
        ],
        compiler_params=pltpu.CompilerParams(vmem_limit_bytes=48 * 1024 * 1024),
        name="atoms",
    )(dens, gy, gyb, pw, pwb, core_wide, weight_wide)
    return ham, energy[:1]

def per_device(dens_part, counts, gaunt, pair_waves, y_table, core, radial_weights):
    band_count = lax.axis_size("band")
    domain_count = lax.axis_size("domain")
    workers = band_count * domain_count
    axes = ("domain", "band")
    me = lax.axis_index("domain") * band_count + lax.axis_index("band")
    entries = dens_part.shape[1]
    slot_total = dens_part.shape[2]
    share = slot_total // band_count
    capacity = -(-share // workers)
    worker_rows = -(-(slot_total // 3) // band_count)
    atoms = round_up(worker_rows, LANES)
    tables = prepare(gaunt, pair_waves, y_table, core, radial_weights)

    own_cols = lax.psum_scatter(dens_part[0], "band", scatter_dimension=1, tiled=True)
    every_count = lax.all_gather(counts, "domain", axis=0, tiled=True)
    band_ids = jnp.arange(band_count, dtype=jnp.int32)
    live = jnp.clip(every_count[:, None] - band_ids[None, :] * share, 0, share).reshape(-1)
    ids = jnp.arange(workers, dtype=jnp.int32)
    starts = jnp.sum(jnp.where(ids[None, :] < ids[:, None], live[None, :], 0), axis=1)
    ends = starts + live
    own_start = jnp.sum(jnp.where(ids == me, starts, 0))
    own_live = jnp.sum(jnp.where(ids == me, live, 0))
    is_alive = jnp.arange(share, dtype=jnp.int32) < own_live

    own_cols = jnp.where(is_alive[None, :], own_cols, 0.0)
    own_cols = jnp.pad(own_cols, ((0, 0), (0, capacity * workers - share)))
    blocks = own_cols.T.reshape(capacity, workers, entries).transpose(1, 0, 2)
    outgoing = jnp.roll(blocks, own_start % workers, axis=0)
    incoming = lax.all_to_all(outgoing, axes, split_axis=0, concat_axis=0, tiled=True)

    atom_ids = jnp.arange(atoms, dtype=jnp.int32) * workers + me
    source = jnp.sum((ends[None, :] <= atom_ids[:, None]).astype(jnp.int32), axis=1)
    source = jnp.minimum(source, workers - 1)
    source_start = jnp.sum(jnp.where(source[:, None] == ids[None, :], starts[None, :], 0), axis=1)
    position = jnp.clip((atom_ids - source_start) // workers, 0, capacity - 1)
    compact = jnp.take(
        incoming.reshape(workers * capacity, entries), source * capacity + position, axis=0,
        mode="clip",
    )
    ham, energy = local_energy(compact.T, tables, pair_waves.shape[0])
    result = jnp.concatenate([ham, energy], axis=0).T
    row = (me - starts) % workers
    first = (starts + row - me) // workers
    target = first[:, None] + jnp.arange(capacity, dtype=jnp.int32)[None, :]
    back = jnp.take(result, jnp.clip(target, 0, atoms - 1).reshape(-1), axis=0, mode="clip")
    returned = lax.all_to_all(
        back.reshape(workers, capacity, entries + 1), axes, split_axis=0, concat_axis=0, tiled=True
    )
    returned = jnp.roll(returned, -(own_start % workers), axis=0)
    final = returned.transpose(1, 0, 2).reshape(capacity * workers, entries + 1).T[:, :share]
    final = jnp.where(is_alive[None, :], final, 0.0)
    whole = lax.all_gather(final, "band", axis=1, tiled=True)
    return whole[:entries], whole[entries]

def solution(mesh):
    return jax.shard_map(
        per_device,
        mesh=mesh,
        in_specs=(P("band", None, "domain"), P("domain"), P(), P(), P(), P(), P()),
        out_specs=(P(None, "domain"), P("domain")),
        check_vma=False,
    )
```

```python
import math

import jax
import jax.numpy as jnp
from jax import lax
from jax.experimental import pallas as pl
from jax.experimental.pallas import tpu as pltpu
from jax.sharding import PartitionSpec as P

highest = lax.Precision.HIGHEST
f32 = jnp.float32
bf16 = jnp.bfloat16

LANES = 128
WIDE = 256

C_RS = 0.6203504908994
EX_A = 0.7385587663820224
EX_D = 0.9847450218426965

def round_up(value, step):
    return -(-value // step) * step

def split(x):
    hi = lax.reduce_precision(x, 8, 7)
    return hi.astype(bf16), (x - hi).astype(bf16)

def atom_kernel(
    dens_ref, gy_ref, gyb_ref, pw_ref, pwb_ref, core_ref, weight_ref,
    ham_ref, energy_ref, pts_ref, hi_ref, lo_ref, eacc_ref, back_ref, *, pairs, step
):
    atoms = dens_ref.shape[1]
    rows = pw_ref.shape[1]
    grid_points = pw_ref.shape[0]
    couples = gy_ref.shape[0]
    chunks = 2 * atoms // WIDE
    eacc_ref[...] = jnp.zeros_like(eacc_ref)

    def mixed(x):
        ids = lax.broadcasted_iota(jnp.int32, x.shape, 0)
        hi = x.astype(bf16).astype(f32)
        low = (ids >= pairs) & (ids < 2 * pairs)
        return jnp.where(low, x - hi, hi).astype(bf16)

    def body(m, carry):
        both = jnp.dot(gy_ref[m], dens_ref[...], preferred_element_type=f32)
        lhs = mixed(jnp.concatenate([both[:rows], both[rows:]], axis=1))
        back = []
        for j in range(chunks):
            cols = lhs[:, j * WIDE:(j + 1) * WIDE]
            pts_ref[j] = jnp.dot(pw_ref[...], cols, preferred_element_type=f32)
            for g in range(0, grid_points, step):
                part = pl.ds(g, step)
                p = pts_ref[j, part, :] + core_ref[part, :]
                u = p * p + 0.25
                v = jnp.exp2(jnp.log(u) * (-1.0 / (6.0 * math.log(2.0))))
                r = v / (7.8 + C_RS * v)
                v2 = v * v
                br = 0.44 * r
                eacc_ref[j, part, :] += (u * v2) * (EX_A + br)
                pot = (p * v2) * (EX_D + (0.44 + (0.44 * C_RS / 3.0) * r) * r)
                hi = pot.astype(bf16)
                hi_ref[j, part, :] = hi
                lo_ref[j, part, :] = (pot - hi.astype(f32)).astype(bf16)
            first = jnp.dot(pwb_ref[...], hi_ref[j], preferred_element_type=f32)
            second = jnp.dot(pwb_ref[:rows, :], lo_ref[j], preferred_element_type=f32)
            back.append(first[:rows] + first[rows:] + second)
        back = mixed(jnp.concatenate(back, axis=1))
        start = pl.multiple_of(m * 2 * rows, 2 * rows)
        back_ref[pl.ds(start, rows), :] = back[:, :atoms]
        back_ref[pl.ds(start + rows, rows), :] = back[:, atoms:]
        return carry

    lax.fori_loop(0, couples, body, 0)
    ham_ref[...] = jnp.dot(gyb_ref[...], back_ref[...], preferred_element_type=f32)
    sums = [
        jnp.sum(eacc_ref[j] * weight_ref[...], axis=0, keepdims=True) for j in range(chunks)
    ]
    sums = jnp.concatenate(sums, axis=1)
    energy_ref[...] = jnp.broadcast_to(
        -(sums[:, :atoms] + sums[:, atoms:]), energy_ref.shape
    )

def prepare(gaunt, pair_waves, y_table, core, radial_weights):
    entries = gaunt.shape[0]
    harmonics, directions = y_table.shape
    pairs, grid_points = pair_waves.shape
    rows = round_up(3 * pairs, 16)
    extra = rows - 3 * pairs
    assert directions % 2 == 0
    fused = jnp.einsum(
        "plq,ln->nqp", gaunt.reshape(entries, harmonics, pairs), y_table, precision=highest
    )

    hi, lo = split(fused)
    wide = lambda a, b, c: jnp.pad(
        jnp.concatenate([a, b, c], axis=1), ((0, 0), (0, extra), (0, 0))
    )
    hi3 = wide(hi, hi, hi)
    lo3 = wide(lo, lo, lo)
    gy = jnp.concatenate([hi3, hi3, lo3], axis=2).reshape(directions // 2, 2 * rows, 3 * entries)
    gyb = wide(hi, hi, lo).reshape(directions * rows, entries).T
    pw_hi, pw_lo = split(pair_waves)
    pw = jnp.pad(jnp.concatenate([pw_hi, pw_hi, pw_lo], axis=0), ((0, extra), (0, 0))).T
    point_weight = 4.0 * jnp.pi / directions * radial_weights
    b_hi, b_lo = split(-point_weight[None, :] * pair_waves)
    triple = lambda x: jnp.pad(jnp.concatenate([x, x, x], axis=0), ((0, extra), (0, 0)))
    pwb = jnp.concatenate([triple(b_hi), triple(b_lo)], axis=0)
    core_wide = jnp.broadcast_to(core[:, None], (grid_points, WIDE))
    weight_wide = jnp.broadcast_to(point_weight[:, None], (grid_points, WIDE))
    return gy, gyb, pw, pwb, core_wide, weight_wide

def local_energy(columns, tables, pairs):
    entries, atoms = columns.shape
    gy, gyb, pw, pwb, core_wide, weight_wide = tables
    grid_points, rows = pw.shape
    hi, lo = split(columns)
    dens = jnp.concatenate([hi, lo, hi], axis=0)
    chunks = 2 * atoms // WIDE
    step = 80 if grid_points % 80 == 0 else grid_points

    ham, energy = pl.pallas_call(
        lambda *refs: atom_kernel(*refs, pairs=pairs, step=step),
        out_shape=(
            jax.ShapeDtypeStruct((entries, atoms), f32),
            jax.ShapeDtypeStruct((8, atoms), f32),
        ),
        scratch_shapes=[
            pltpu.VMEM((chunks, grid_points, WIDE), f32),
            pltpu.VMEM((chunks, grid_points, WIDE), bf16),
            pltpu.VMEM((chunks, grid_points, WIDE), bf16),
            pltpu.VMEM((chunks, grid_points, WIDE), f32),
            pltpu.VMEM((gyb.shape[1], atoms), bf16),
        ],
        compiler_params=pltpu.CompilerParams(vmem_limit_bytes=48 * 1024 * 1024),
        name="atoms",
    )(dens, gy, gyb, pw, pwb, core_wide, weight_wide)
    return ham, energy[:1]

def per_device(dens_part, counts, gaunt, pair_waves, y_table, core, radial_weights):
    band_count = lax.axis_size("band")
    domain_count = lax.axis_size("domain")
    workers = band_count * domain_count
    axes = ("domain", "band")
    me = lax.axis_index("domain") * band_count + lax.axis_index("band")
    entries = dens_part.shape[1]
    slot_total = dens_part.shape[2]
    share = slot_total // band_count
    capacity = -(-share // workers)
    worker_rows = -(-(slot_total // 3) // band_count)
    atoms = round_up(worker_rows, LANES)
    tables = prepare(gaunt, pair_waves, y_table, core, radial_weights)

    own_cols = lax.psum_scatter(dens_part[0], "band", scatter_dimension=1, tiled=True)
    every_count = lax.all_gather(counts, "domain", axis=0, tiled=True)
    band_ids = jnp.arange(band_count, dtype=jnp.int32)
    live = jnp.clip(every_count[:, None] - band_ids[None, :] * share, 0, share).reshape(-1)
    ids = jnp.arange(workers, dtype=jnp.int32)
    starts = jnp.sum(jnp.where(ids[None, :] < ids[:, None], live[None, :], 0), axis=1)
    ends = starts + live
    own_start = jnp.sum(jnp.where(ids == me, starts, 0))
    own_live = jnp.sum(jnp.where(ids == me, live, 0))
    is_alive = jnp.arange(share, dtype=jnp.int32) < own_live

    own_cols = jnp.where(is_alive[None, :], own_cols, 0.0)
    own_cols = jnp.pad(own_cols, ((0, 0), (0, capacity * workers - share)))
    blocks = own_cols.T.reshape(capacity, workers, entries).transpose(1, 0, 2)
    outgoing = jnp.roll(blocks, own_start % workers, axis=0)
    incoming = lax.all_to_all(outgoing, axes, split_axis=0, concat_axis=0, tiled=True)

    atom_ids = jnp.arange(atoms, dtype=jnp.int32) * workers + me
    source = jnp.sum((ends[None, :] <= atom_ids[:, None]).astype(jnp.int32), axis=1)
    source = jnp.minimum(source, workers - 1)
    source_start = jnp.sum(jnp.where(source[:, None] == ids[None, :], starts[None, :], 0), axis=1)
    position = jnp.clip((atom_ids - source_start) // workers, 0, capacity - 1)
    compact = jnp.take(
        incoming.reshape(workers * capacity, entries), source * capacity + position, axis=0,
        mode="clip",
    )
    ham, energy = local_energy(compact.T, tables, pair_waves.shape[0])
    result = jnp.concatenate([ham, energy], axis=0).T
    row = (me - starts) % workers
    first = (starts + row - me) // workers
    target = first[:, None] + jnp.arange(capacity, dtype=jnp.int32)[None, :]
    back = jnp.take(result, jnp.clip(target, 0, atoms - 1).reshape(-1), axis=0, mode="clip")
    returned = lax.all_to_all(
        back.reshape(workers, capacity, entries + 1), axes, split_axis=0, concat_axis=0, tiled=True
    )
    returned = jnp.roll(returned, -(own_start % workers), axis=0)
    piece = returned.transpose(1, 0, 2).reshape(capacity * workers, entries + 1)[:share]
    piece = jnp.where(is_alive[:, None], piece, 0.0)
    band = lax.axis_index("band")
    whole = jnp.zeros((slot_total, entries + 1), f32)
    ring = [(i, (i + 1) % band_count) for i in range(band_count)]
    for hop in range(band_count):
        owner = (band - hop) % band_count
        whole = lax.dynamic_update_slice(whole, piece, (owner * share, 0))
        if hop + 1 < band_count:
            piece = lax.ppermute(piece, "band", ring)
    whole = whole.T
    return whole[:entries], whole[entries]

def solution(mesh):
    return jax.shard_map(
        per_device,
        mesh=mesh,
        in_specs=(P("band", None, "domain"), P("domain"), P(), P(), P(), P(), P()),
        out_specs=(P(None, "domain"), P("domain")),
        check_vma=False,
    )
```
